32 devices in a mesh: gx: 4 (over z), gy: 2 (over x), gz: 4 (over y, core).
Axes of the slice: x: 2, y: 2, z: 4, core: 2. Of those that a mesh axis runs over, the one named last changes fastest.
Arguments:
- attn_out: bfloat16 [16384, 8192], P('gx', ('gy', 'gz')), may hold values from -6 to 6
- out_grad: bfloat16 [16384, 8192], P('gx', ('gz', 'gy')), may hold values from -0.046875 to 0.046875
- valid_counts: int32 [16], P('gx'), may hold values from 128 to 1024
Outputs:
- weight_grad: float32 [8192, 8192], P(('gy', 'gx'), 'gz')
The draws below stay inside these ranges and needn't reach their ends.
Inputs may be any that keep to these rules, and one draw needn't show every extreme that they name: `valid_counts`: valid tokens of a packed row come first, padding after.
All inputs are finite; a program needn't handle non-finite values.
Results may differ from the reference program's by a relative error of at most 0.0003.
Values may be sent and summed in bfloat16 or wider, within the bound.
No kernel may reach another device: no remote copies, remote signals or barrier semaphores. Data moves between devices by JAX's collectives and lax.ppermute only.
A program may use at most 192 MiB of HBM per device.

```python
import jax
import jax.numpy as jnp
from jax import lax

D = 8192
HD = 8192
SEQ = 1024
ROWS = 16
TOKENS = 16384


def set_ends(drawn, rng, smallest, high):
    place = [jax.random.randint(jax.random.fold_in(rng, axis), (), 0, length) for axis, length in enumerate(drawn.shape)]
    main_axis = drawn.shape.index(max(drawn.shape))
    beside = place[:main_axis] + [(place[main_axis] + 1) % drawn.shape[main_axis]] + place[main_axis + 1:]
    return drawn.at[tuple(place)].set(smallest).at[tuple(beside)].set(high)


def raised(values, key, source, target, shards_of, factor):
    owner, partner = [(jnp.arange(values.shape[position]) // (values.shape[position] // shards_of)).reshape([-1 if axis == position else 1 for axis in range(values.ndim)]) for position in (source, target)]
    chosen = jax.random.permutation(key, shards_of)[partner]
    strong = (owner == chosen) | (owner == (partner + shards_of // 2) % shards_of)
    return jnp.where(strong, factor * values, values)


def level_of(stream_key, shape, split, least, largest):
    factor_of = 1.0
    for position, blocks in split:
        draws = jax.random.uniform(jax.random.fold_in(jax.random.fold_in(stream_key, 6), position), (blocks,), jnp.float32, least / len(split), largest / len(split))
        factor_of = factor_of * jnp.repeat(jnp.exp(draws), shape[position] // blocks).reshape((-1,) + (1,) * (len(shape) - 1 - position))
    return factor_of


def scatter_about(stream_key, dims, spread, bound, shards=(), kind=jnp.bfloat16):
    factor_of = level_of(stream_key, dims, shards, -0.22, 0.18) if shards else 1.0
    result = jax.random.normal(stream_key, dims, jnp.float32) * spread * factor_of
    return jnp.minimum(jnp.maximum(result, -bound), bound).astype(kind)


def heavy_noise(rng, dims, deviation, reach, shards, heavy, kind=jnp.bfloat16):
    result = deviation * jax.random.normal(rng, dims, jnp.float32)
    if shards:
        result = result * level_of(rng, dims, shards, -0.22, 0.18)
    return jnp.clip(raised(result, jax.random.fold_in(rng, 3), *heavy), -reach, reach).astype(kind)


def setup_inputs(seed: int = 0) -> dict:
    arg_keys = jax.random.split(jax.random.key(seed), 4)
    attn_out = heavy_noise(arg_keys[0], (TOKENS, HD), 1.0, 6.0, ((0, 4), (1, 8)), (0, 1, 8, 2.0))
    out_grad = scatter_about(arg_keys[1], (TOKENS, D), (TOKENS ** -0.5), 0.046875, ((0, 4), (1, 8)))
    valid_counts = set_ends(jax.random.randint(arg_keys[2], (ROWS,), SEQ // 8, SEQ + 1), jax.random.fold_in(arg_keys[2], 1), SEQ // 8, SEQ).astype(jnp.int32)
    return {"attn_out": attn_out, "out_grad": out_grad, "valid_counts": valid_counts}


def reference(attn_out, out_grad, valid_counts):
    positions = jnp.arange(SEQ, dtype=jnp.int32)
    kept_rows = (positions[None, :] < valid_counts[:, None]).reshape(-1)
    masked = jnp.where(kept_rows[:, None], out_grad, jnp.zeros((), out_grad.dtype))
    return lax.dot_general(attn_out, masked, (((0,), (0,)), ((), ())), preferred_element_type=jnp.float32)
```

```python
import functools

import jax
import jax.numpy as jnp
import numpy as np
from jax import lax
from jax.experimental import pallas as pl
from jax.experimental.pallas import tpu as pltpu
from jax.sharding import PartitionSpec as P


GROUP = 128
STEPS = 64.0
TOP = 32700.0
EXTRA = 16
DELAY = 2
IDLE, SEND, FORWARD, FIRST, SECOND = range(5)
FIELDS = 6


def sending_order(near, far):
    first = [(d, 0, c) for d in near for c in range(2)]
    second = [(d, 0, 0) for d in far] + [(d, 1, 0) for d in near]
    third = [(d, 0, 1) for d in far] + [(d, 1, c) for d in far for c in range(2)] + [(d, 1, 1) for d in near]
    return first, second, third


def by_distance(stage, depth):
    return sorted(stage, key=depth, reverse=True)


def line_orders(n, near):
    far = [d for d in range(n) if d not in near]
    up = sending_order([d for d in near if d > 0], [d for d in far if d > 0])
    down = sending_order([d for d in near if d < n - 1], [d for d in far if d < n - 1])
    up = [by_distance(stage, lambda c: c[0]) for stage in up]
    down = [by_distance(stage, lambda c: n - 1 - c[0]) for stage in down]
    most = max(len(up[0]), len(down[0]))
    for stages in (up, down):
        if 2 * len(stages[0]) == most:
            stages[0] = [c for pair in stages[0] for c in (pair, None)]
    return [c for stage in up for c in stage], [c for stage in down for c in stage]


def plan(n, nz):
    orders = []
    for lane in range(nz):
        near = sorted({lane, lane ^ 1})
        orders.append(line_orders(n, near))
    ends = [(lst, end) for o in orders for lst, end in zip(o, (0, n - 1))]
    rounds = max(i + DELAY * abs(c[0] - end) for lst, end in ends for i, c in enumerate(lst) if c is not None) + 1
    modes = np.zeros((rounds, 2, n, nz), np.int64)
    chunks = np.zeros((rounds, 2, n, nz, 3), np.int64)
    for lane in range(nz):
        seen = set()
        for i in range(rounds):
            for slot in range(2):
                lst = orders[lane][slot]
                for z in range(n):
                    place = z if slot == 0 else n - 1 - z
                    at = i - DELAY * place
                    if not 0 <= at < len(lst) or lst[at] is None:
                        continue
                    d, j, c = lst[at]
                    left = d - z if slot == 0 else z - d
                    if left < 0:
                        continue
                    if left > 0:
                        mode = SEND if place == 0 else FORWARD
                    else:
                        mode = SECOND if (d, j, c) in seen else FIRST
                        seen.add((d, j, c))
                    modes[i, slot, z, lane] = mode
                    chunks[i, slot, z, lane] = d, j, c
    return rounds, modes, chunks


def cells_of(number):
    if number < 2:
        return [(2 * number, r, c) for r in range(2) for c in range(2)]
    if number < 6:
        p, across = divmod(number - 2, 2)
        return [(4, p, c) for c in range(2)] + [(6, p, c) for c in range(2)] if across else [(blk, r, p) for blk in (1, 3) for r in range(2)]
    return [(5 + 2 * (number - 6), r, c) for r in range(2) for c in range(2)]


def sequence(n, nz):
    rounds, modes, chunks = plan(n, nz)
    first = {}
    for i, s, z, b in np.ndindex(rounds, 2, n, nz):
        if modes[i, s, z, b] in (SEND, FORWARD, FIRST):
            d, j, c = chunks[i, s, z, b]
            for t in range(2):
                first.setdefault(((b ^ d) * 2 + j, c if j == 0 else t, t if j == 0 else c), i)
    due = [min(first[tuple(int(v) for v in cell)] for cell in cells_of(number)) for number in range(8)]
    for stage in ((2, 3), (4, 5, 6, 7)):
        for place, number in enumerate(stage):
            due[number] = min(due[k] for k in stage[place:])
    steps = []
    for i in range(rounds):
        steps += [("product", number) for number in range(8) if due[number] == i]
        steps.append(("round", i))
    return steps


def product_kernel(n_a, n_g, places, block, counts, ids, limits, *refs):
    a_refs, g_refs = refs[:n_a], refs[n_a : n_a + n_g]
    out_ref, acc, sem = refs[-3:]
    step = pl.program_id(0)
    n_rows, n_cols = a_refs[0].shape[1], g_refs[0].shape[1]

    @pl.when(step == 0)
    def _():
        acc[...] = jnp.zeros_like(acc)

    @pl.when(step < counts[0])
    def _():
        inside = lax.broadcasted_iota(jnp.int32, (block, 1), 0) < limits[step]
        for c in range(n_g):
            g = jnp.where(inside, g_refs[c][...], jnp.zeros((), g_refs[c].dtype))
            for r in range(n_a):
                acc[r, c] += lax.dot_general(
                    a_refs[r][...], g, (((0,), (0,)), ((), ())), preferred_element_type=jnp.float32
                )

    @pl.when(step == pl.num_programs(0) - 1)
    def _():
        copies = []
        for r in range(n_a):
            for c in range(n_g):
                blk, r0, c0 = places[r][c]
                target = out_ref.at[blk, pl.ds(r0, n_rows), pl.ds(c0, n_cols)]
                copies.append(pltpu.make_async_copy(acc.at[r, c], target, sem.at[r * n_g + c]))
                copies[-1].start()
        for copy in copies:
            copy.wait()


def product(tables, block, heads, grads, places, partials):
    tokens = heads[0].shape[0]
    rows, cols = heads[0].shape[1], grads[0].shape[1]
    n_a, n_g = len(heads), len(grads)
    at = lambda i, counts, ids, limits: (ids[i], 0)
    specs = [pl.BlockSpec((block, x.shape[1]), at) for x in (*heads, *grads)]
    fresh = isinstance(partials, jax.ShapeDtypeStruct)
    if not fresh:
        specs.append(pl.BlockSpec(memory_space=pl.ANY))
    return pl.pallas_call(
        functools.partial(product_kernel, n_a, n_g, places, block),
        grid_spec=pltpu.PrefetchScalarGridSpec(
            num_scalar_prefetch=3,
            grid=(tokens // block,),
            in_specs=specs,
            out_specs=pl.BlockSpec(memory_space=pl.ANY),
            scratch_shapes=[
                pltpu.VMEM((n_a, n_g, rows, cols), jnp.float32),
                pltpu.SemaphoreType.DMA((n_a * n_g,)),
            ],
        ),
        out_shape=jax.ShapeDtypeStruct(partials.shape, partials.dtype),
        input_output_aliases={} if fresh else {3 + n_a + n_g: 0},
        compiler_params=pltpu.CompilerParams(vmem_limit_bytes=56 << 20),
        cost_estimate=pl.CostEstimate(
            flops=2 * tokens * rows * cols * n_a * n_g, bytes_accessed=tokens * 2 * (rows * n_a + cols * n_g), transcendentals=0
        ),
        name="product",
    )(*tables, *heads, *grads, *([] if fresh else [partials]))


def encode(x_ref, q_ref, tile, rows, add):
    cols = x_ref.shape[1]

    slots = lax.broadcasted_iota(jnp.int32, (EXTRA, cols), 0)

    def group(g, marks):
        at = pl.ds(pl.multiple_of(g * GROUP, GROUP), GROUP)
        x = x_ref[at, :]
        if add is not None:
            x = x + add(g)
        largest = jnp.max(jnp.abs(x), axis=0, keepdims=True)
        mark = jnp.ceil(jnp.log2(jnp.maximum(largest, 1e-30)) * STEPS)
        inverse = jnp.exp2(mark * (-1.0 / STEPS)) * TOP
        q_ref[tile, at, :] = jnp.round(x * inverse).astype(jnp.int32).astype(jnp.int16)
        return jnp.where(slots == g, mark.astype(jnp.int32), marks)

    marks = lax.fori_loop(0, rows // GROUP, group, jnp.zeros((EXTRA, cols), jnp.int32))
    q_ref[tile, pl.ds(rows, EXTRA), :] = marks.astype(jnp.int16)


def decode(r_ref, tile, rows, g):
    cols = r_ref.shape[2]
    marks = r_ref[tile, pl.ds(rows, EXTRA), :].astype(jnp.int32)
    slots = lax.broadcasted_iota(jnp.int32, (EXTRA, cols), 0)
    mark = jnp.sum(jnp.where(slots == g, marks, 0), axis=0, keepdims=True).astype(jnp.float32)
    scale = jnp.exp2(mark * (1.0 / STEPS)) * (1.0 / TOP)
    q = r_ref[tile, pl.ds(pl.multiple_of(g * GROUP, GROUP), GROUP), :].astype(jnp.int32).astype(jnp.float32)
    return q * scale


def round_kernel(index, sends, recvs, side, roles, *refs):
    n_recv, n_send = sum(recvs), sum(sends)
    recv_refs = list(refs[:n_recv])
    outs = list(refs[-9 - n_send : -9])
    partials, out, p_tile, r_tile, q_tile, sem_p, sem_r, sem_q, sem_o = refs[-9:]
    recv_of = [recv_refs.pop(0) if has else None for has in recvs]
    send_of = [outs.pop(0) if has else None for has in sends]

    def role(slot, field):
        return roles[(index * 2 + slot) * FIELDS + field]

    def p_copy(slot, t):
        r0, c0 = role(slot, 2), role(slot, 3)
        along_rows = role(slot, 1) % 2
        r0 = pl.multiple_of(r0 + t * side * along_rows, side)
        c0 = pl.multiple_of(c0 + t * side * (1 - along_rows), side)
        source = partials.at[role(slot, 1), pl.ds(r0, side), pl.ds(c0, side)]
        return pltpu.make_async_copy(source, p_tile.at[slot, t], sem_p.at[slot, t])

    def o_place(slot, t):
        along_rows = role(slot, 1) % 2
        r0 = pl.multiple_of(role(slot, 4) + t * side * along_rows, side)
        c0 = pl.multiple_of(role(slot, 5) + t * side * (1 - along_rows), side)
        return out.at[pl.ds(r0, side), pl.ds(c0, side)]

    def r_copy(slot):
        return pltpu.make_async_copy(recv_of[slot], r_tile.at[slot], sem_r.at[slot])

    def q_copy(slot):
        return pltpu.make_async_copy(q_tile.at[slot], send_of[slot], sem_q.at[slot])

    for slot in range(2):
        mode = role(slot, 0)

        @pl.when((mode != IDLE) & (mode != SECOND))
        def _():
            for t in range(2):
                p_copy(slot, t).start()

        if recvs[slot]:

            @pl.when(mode >= FORWARD)
            def _():
                r_copy(slot).start()

    for slot in range(2):
        mode = role(slot, 0)
        if sends[slot]:

            @pl.when(mode == SEND)
            def _():
                for t in range(2):
                    p_copy(slot, t).wait()
                    encode(p_tile.at[slot, t], q_tile.at[slot], t, side, None)
                q_copy(slot).start()

            if recvs[slot]:

                @pl.when(mode == FORWARD)
                def _():
                    r_copy(slot).wait()
                    for t in range(2):
                        p_copy(slot, t).wait()
                        encode(
                            p_tile.at[slot, t], q_tile.at[slot], t, side, functools.partial(decode, r_tile.at[slot], t, side)
                        )
                    q_copy(slot).start()

        if recvs[slot]:

            @pl.when(mode >= FIRST)
            def _():
                r_copy(slot).wait()
                for t in range(2):

                    @pl.when(mode == FIRST)
                    def _():
                        p_copy(slot, t).wait()

                    @pl.when(mode == SECOND)
                    def _():
                        back = pltpu.make_async_copy(o_place(slot, t), p_tile.at[slot, t], sem_p.at[slot, t])
                        back.start()
                        back.wait()

                    def add(g, _):
                        at = pl.ds(pl.multiple_of(g * GROUP, GROUP), GROUP)
                        p_tile[slot, t, at, :] += decode(r_tile.at[slot], t, side, g)
                        return 0

                    lax.fori_loop(0, side // GROUP, add, 0)
                    pltpu.make_async_copy(p_tile.at[slot, t], o_place(slot, t), sem_o.at[slot, t]).start()
                for t in range(2):
                    pltpu.make_async_copy(p_tile.at[slot, t], o_place(slot, t), sem_o.at[slot, t]).wait()

    for slot in range(2):
        if sends[slot]:

            @pl.when((role(slot, 0) == SEND) | (role(slot, 0) == FORWARD))
            def _():
                q_copy(slot).wait()


def one_round(index, side, roles, sends, received, partials, out):
    height = side + EXTRA
    recvs = tuple(r is not None for r in received)
    arrays = [r for r in received if r is not None]
    sent = jax.ShapeDtypeStruct((2, height, side), jnp.int16)
    n_send, n_recv = sum(sends), len(arrays)
    hbm = pl.BlockSpec(memory_space=pl.ANY)
    carried = [partials] if isinstance(out, jax.ShapeDtypeStruct) else [partials, out]
    results = pl.pallas_call(
        functools.partial(round_kernel, index, sends, recvs, side),
        grid_spec=pltpu.PrefetchScalarGridSpec(
            num_scalar_prefetch=1,
            grid=(),
            in_specs=[hbm] * (n_recv + len(carried)),
            out_specs=[hbm] * (n_send + 2),
            scratch_shapes=[
                pltpu.VMEM((2, 2, side, side), jnp.float32),
                pltpu.VMEM((2, 2, height, side), jnp.int16),
                pltpu.VMEM((2, 2, height, side), jnp.int16),
                pltpu.SemaphoreType.DMA((2, 2)),
                pltpu.SemaphoreType.DMA((2,)),
                pltpu.SemaphoreType.DMA((2,)),
                pltpu.SemaphoreType.DMA((2, 2)),
            ],
        ),
        out_shape=[sent] * n_send
        + [jax.ShapeDtypeStruct(partials.shape, partials.dtype), jax.ShapeDtypeStruct(out.shape, out.dtype)],
        input_output_aliases={1 + n_recv + i: n_send + i for i in range(len(carried))},
        compiler_params=pltpu.CompilerParams(vmem_limit_bytes=24 << 20),
        cost_estimate=pl.CostEstimate(flops=4 * side * side * 1000, bytes_accessed=32 * side * side, transcendentals=0),
        name="round",
    )(roles, *arrays, *carried)
    sent = list(results[:n_send])
    return [sent.pop(0) if has else None for has in sends], results[-2], results[-1]


def token_tables(valid_counts, slot_count, block):
    per_row = slot_count // block
    starts = jnp.arange(per_row, dtype=jnp.int32) * block
    left = jnp.clip(valid_counts[:, None] - starts[None, :], 0, block).reshape(-1)
    total = left.shape[0]
    order = jnp.cumsum((left > 0).astype(jnp.int32)) - 1
    count = order[-1] + 1
    wanted = jnp.minimum(jnp.arange(total, dtype=jnp.int32), count - 1)
    chosen = (order[None, :] == wanted[:, None]) & (left > 0)[None, :]
    ids = jnp.sum(jnp.where(chosen, jnp.arange(total, dtype=jnp.int32)[None, :], 0), axis=1)
    limits = jnp.sum(jnp.where(chosen, left[None, :], 0), axis=1)
    return count.reshape(1), ids, limits


def line_shards(n, ny, nz, attn_out, out_grad, valid_counts):
    tokens, m = attn_out.shape
    side = m // 2
    slot_count = tokens // valid_counts.shape[0]
    block = min(512, slot_count)
    tables = token_tables(valid_counts, slot_count, block)
    z, y, lane = (lax.axis_index(a) for a in ("gx", "gy", "gz"))

    rounds, modes, chunks = plan(n, nz)
    static = np.zeros((n, ny, nz, rounds, 2, FIELDS), np.int32)
    for i, s, zz, b in np.ndindex(rounds, 2, n, nz):
        d, j, c = chunks[i, s, zz, b]
        r0, c0 = (c * side, 0) if j == 0 else (0, c * side)
        for yy in range(ny):
            static[zz, yy, b, i, s] = modes[i, s, zz, b], (b ^ d) * 2 + j, r0, c0, r0, c0 + (yy ^ j) * m
    roles = jnp.asarray(static.reshape(n * ny * nz, -1))[(z * ny + y) * nz + lane]

    def swap(x, axis, size, bits):
        return lax.ppermute(x, axis, [(i, i ^ bits) for i in range(size)])

    halves = lambda x: [x[:, :side], x[:, side:]]
    beside = swap(attn_out, "gz", nz, 1)
    grad_halves, head_halves = [], []
    for p, (g, a) in enumerate(zip(halves(out_grad), halves(attn_out))):
        head_halves.append([swap(a, "gz", nz, 2)])
        grad_halves.append(swap(g, "gy", ny, 1))

    partials = jax.ShapeDtypeStruct((2 * nz, m, m), jnp.float32)
    out = jax.ShapeDtypeStruct((m, ny * m), jnp.float32)
    near, far = [attn_out, beside], head_halves
    quarters = [[(0, 0), (0, side)], [(side, 0), (side, side)]]

    def operands(number):
        if number < 2:
            return near[number : number + 1], [out_grad], [[(2 * number, 0, 0)]]
        if number < 6:
            p, across = divmod(number - 2, 2)
            at = p * side
            if across:
                return far[p], [out_grad], [[(4, at, 0)], [(6, at, 0)]]
            return near, [grad_halves[p]], [[(1, 0, at)], [(3, 0, at)]]
        k = number - 6
        return [far[0][k], far[1][k]], grad_halves, [[(5 + 2 * k, *q) for q in row] for row in quarters]

    waiting = {}
    for kind, i in sequence(n, nz):
        if kind == "product":
            p = 0 if i == 3 else 1
            if i in (3, 5):
                across, partials = lax.optimization_barrier((far[p][0], partials))
                far[p] = [across, swap(across, "gz", nz, 1)]
            partials = product(tables, block, *operands(i), partials)
            continue
        pairs = [
            [
                (zz * nz + b, (zz + (1, -1)[s]) * nz + b)
                for zz in range(n)
                for b in range(nz)
                if modes[i, s, zz, b] in (SEND, FORWARD)
            ]
            for s in range(2)
        ]
        sends = tuple(bool(p) for p in pairs)
        received = [waiting.pop((i - DELAY, s), None) for s in range(2)]
        sent, partials, out = one_round(i, side, roles, sends, received, partials, out)
        for s in range(2):
            if sends[s]:
                waiting[(i, s)] = lax.ppermute(sent[s], ("gx", "gz"), pairs[s])
    return out


def plain_shards(attn_out, out_grad, valid_counts):
    rows_here = valid_counts.shape[0]
    slot_count = attn_out.shape[0] // rows_here
    positions = lax.broadcasted_iota(jnp.int32, (rows_here, slot_count), 1)
    kept_rows = (positions < valid_counts[:, None]).reshape(-1)
    gathered_inputs = lax.all_gather(attn_out, "gz", axis=1, tiled=True)
    gathered_grads = lax.all_gather(out_grad, "gy", axis=1, tiled=True)
    masked = jnp.where(kept_rows[:, None], gathered_grads, jnp.zeros((), gathered_grads.dtype))
    partial_grad = lax.dot_general(
        gathered_inputs, masked, (((0,), (0,)), ((), ())), preferred_element_type=jnp.float32
    )
    return lax.psum_scatter(partial_grad, "gx", scatter_dimension=0, tiled=True)


def solution(mesh):
    nx, ny, nz = (mesh.shape[a] for a in ("gx", "gy", "gz"))

    def shards(attn_out, out_grad, valid_counts):
        square = attn_out.shape[1] == out_grad.shape[1] and attn_out.shape[1] % (2 * GROUP) == 0
        if nx == nz == 4 and ny == 2 and square:
            return line_shards(nx, ny, nz, attn_out, out_grad, valid_counts)
        return plain_shards(attn_out, out_grad, valid_counts)

    in_specs = (P("gx", ("gy", "gz")), P("gx", ("gz", "gy")), P("gx"))
    out_specs = P(("gy", "gx"), "gz")
    return jax.shard_map(shards, mesh=mesh, in_specs=in_specs, out_specs=out_specs, check_vma=False)
```
